32 devices in a mesh: lat: 4 (over y, x), lon: 8 (over z, core).
Axes of the slice: x: 2, y: 2, z: 4, core: 2. Of those that a mesh axis runs over, the one named last changes fastest.
Arguments:
- activations: bfloat16 [4, 16, 720, 512], P(None, 'lat', 'lon'), may hold values from -48 to 48
- upstream: bfloat16 [4, 16, 720, 512], P(None, 'lat', 'lon'), may hold values from -6 to 6
- master: float32 [512, 9, 512], P(('lat', 'lon')), may hold values from -0.09375 to 0.09375
- moment_one: float32 [512, 9, 512], P(('lat', 'lon')), may hold values from -2.5 to 2.5
- moment_two: float32 [512, 9, 512], P(('lat', 'lon')), may hold values from 0.01 to 1
Outputs:
- input_grad: bfloat16 [4, 16, 720, 512], P(None, 'lat', 'lon')
- new_weights: bfloat16 [512, 9, 512], replicated
- new_master: float32 [512, 9, 512], P(('lat', 'lon'))
- new_moment_one: float32 [512, 9, 512], P(('lat', 'lon'))
- new_moment_two: float32 [512, 9, 512], P(('lat', 'lon'))
- clipped_grad: float32 [512, 9, 512], P(('lat', 'lon'))
The draws below stay inside these ranges and needn't reach their ends.
All inputs are finite; a program needn't handle non-finite values.
Results may differ from the reference program's by a relative error of at most 0.0049.
Values may be sent and summed in bfloat16 or wider, within the bound.
A program may use at most 128 MiB of HBM per device.

```python
import math
import jax
import jax.numpy as jnp
from jax import lax

CIN = 512
COUT = 512
TAPS = 9
BATCH = 4
COLS_DEV = 90
NLAT = 16
NLON = 720
N_LON = 8


def draw_activations(key, part):
    key_noise, key_spread = jax.random.split(key, 2)
    key_pair = jax.random.fold_in(key, 77)
    channel_ramp = jnp.sqrt(1.0 + 2.0 * jnp.arange(CIN, dtype=jnp.float32) / CIN)
    spread = jnp.exp(jax.random.uniform(key_spread, (CIN,), jnp.float32, 0.0, jnp.log(10.0)))
    chan_scale = channel_ramp * spread / 4.0
    pairing = jax.random.permutation(key_pair, N_LON)
    col_block = jnp.arange(NLON, dtype=jnp.int32) // COLS_DEV
    chan_block = jnp.arange(CIN, dtype=jnp.int32) // (CIN // N_LON)
    heavy = pairing[col_block][:, None] == chan_block[None, :]
    boost = jnp.where(heavy, 6.0, 1.0).astype(jnp.float32)[None, None, :, :]
    noise_draw = jax.random.normal(key_noise, (BATCH, NLAT, NLON, CIN), jnp.float32)
    values = noise_draw * chan_scale * boost
    return jnp.clip(values, -48.0, 48.0).astype(jnp.bfloat16)


def level_of(key, dims, cuts, low, top_value):
    factor_of = 1.0
    for dim, parts in cuts:
        draws = jax.random.uniform(jax.random.fold_in(jax.random.fold_in(key, 6), dim), (parts,), jnp.float32, low / len(cuts), top_value / len(cuts))
        factor_of = factor_of * jnp.repeat(jnp.exp(draws), dims[dim] // parts).reshape((-1,) + (1,) * (len(dims) - 1 - dim))
    return factor_of


def scatter_about(stream_key, extent, deviation, limit, cuts=(), kind=jnp.bfloat16):
    level = level_of(stream_key, extent, cuts, -0.22, 0.18) if cuts else 1.0
    result = jax.random.normal(stream_key, extent, jnp.float32) * deviation * level
    return jnp.minimum(jnp.maximum(result, -limit), limit).astype(kind)


def setup_inputs(seed: int = 0) -> dict:
    key_list = jax.random.split(jax.random.key(seed), 6)
    activations = draw_activations(jax.random.fold_in(key_list[5], 71), 0)
    upstream = scatter_about(key_list[1], (BATCH, NLAT, NLON, COUT), 1.0, 6.0, ((1, 4), (2, 8)))
    master = scatter_about(key_list[2], (CIN, TAPS, COUT), (CIN * TAPS) ** -0.5, 0.09375, ((0, 32),), jnp.float32)
    moment_one = scatter_about(key_list[3], (CIN, TAPS, COUT), 0.3, 2.5, ((0, 32),), jnp.float32)
    moment_two = jnp.clip(jnp.exp(math.log(1.0) - 4.6051702 * jax.random.uniform(key_list[4], (CIN, TAPS, COUT), jnp.float32) ** level_of(key_list[4], (CIN, TAPS, COUT), ((0, 32),), -0.2, 0.2)), 0.01, 1.0)
    return {"activations": activations, "upstream": upstream, "master": master, "moment_one": moment_one, "moment_two": moment_two}


learn_rate = 0.01
beta_one = 0.9
beta_two = 0.999
adam_eps = 1e-08
decay_rate = 0.1
step_count = 10.0
norm_eps = 1e-06

def widen_field(field):
    padded = jnp.pad(field, ((1, 1), (0, 0), (0, 0)))
    return jnp.concatenate([padded[:, -1:, :], padded, padded[:, :1, :]], axis=1)

def reference(activations, upstream, master, moment_one, moment_two):
    weights = master.astype(jnp.bfloat16)

    def one_sample(grad_total, sample):
        act_one, up_one = sample
        act_wide = widen_field(act_one)
        up_wide = widen_field(up_one)
        up_flat = up_one.reshape(-1, COUT)
        data_sum = jnp.zeros((NLAT * NLON, CIN), jnp.float32)
        tap_parts = []
        for tap_index in range(9):
            row_off, col_off = divmod(tap_index, 3)
            shifted = up_wide[2 - row_off:2 - row_off + NLAT, 2 - col_off:2 - col_off + NLON, :].reshape(-1, COUT)
            data_sum = data_sum + jnp.dot(shifted, weights[:, tap_index, :].T, preferred_element_type=jnp.float32)
            act_tap = act_wide[row_off:row_off + NLAT, col_off:col_off + NLON, :].reshape(-1, CIN)
            tap_parts.append(jnp.dot(act_tap.T, up_flat, preferred_element_type=jnp.float32))
        grad_total = grad_total + jnp.stack(tap_parts, axis=1)
        return (grad_total, data_sum.reshape(NLAT, NLON, CIN).astype(jnp.bfloat16))
    grad_total, input_grad = lax.scan(one_sample, jnp.zeros((CIN, 9, COUT), jnp.float32), (activations, upstream))
    max_norm = math.sqrt(float(CIN * TAPS * COUT))
    square_sum = jnp.sum(grad_total * grad_total)
    clip_factor = jnp.minimum(1.0, max_norm / (jnp.sqrt(square_sum) + norm_eps))
    grad_scaled = clip_factor * grad_total
    new_one = beta_one * moment_one + (1.0 - beta_one) * grad_scaled
    new_two = beta_two * moment_two + (1.0 - beta_two) * grad_scaled * grad_scaled
    first_hat = new_one / (1.0 - beta_one ** step_count)
    second_hat = new_two / (1.0 - beta_two ** step_count)
    new_master = master - learn_rate * (first_hat / (jnp.sqrt(second_hat) + adam_eps) + decay_rate * master)
    new_weights = new_master.astype(jnp.bfloat16)
    return (input_grad, new_weights, new_master, new_one, new_two, grad_scaled)
```

```python
import functools
import math

import jax
import jax.numpy as jnp
from jax import lax
from jax.experimental import pallas as pl
from jax.experimental.pallas import tpu as pltpu
from jax.sharding import PartitionSpec as P

MESH = pl.DeviceIdType.MESH

CIN = 512
COUT = 512
TAPS = 9


learn_rate = 0.01
beta_one = 0.9
beta_two = 0.999
adam_eps = 1e-08
decay_rate = 0.1
step_count = 10.0
norm_eps = 1e-06


def halo_kernel(n_lat, n_lon, *refs):
    sources, landings, (send_sem, recv_sem) = refs[:8], refs[8:16], refs[16:]
    lat, lon = lax.axis_index("lat"), lax.axis_index("lon")
    steps = ((-1, 0), (1, 0), (0, -1), (0, 1), (-1, -1), (-1, 1), (1, -1), (1, 1))
    targets = [
        (lax.rem(lat + dy + n_lat, n_lat), lax.rem(lon + dx + n_lon, n_lon)) for dy, dx in steps
    ]
    barrier = pltpu.get_barrier_semaphore()
    for target in targets:
        pl.semaphore_signal(barrier, inc=1, device_id=target, device_id_type=MESH)
    pl.semaphore_wait(barrier, len(targets))
    copies = []
    for index, target in enumerate(targets):
        copy = pltpu.make_async_remote_copy(
            src_ref=sources[index], dst_ref=landings[index], send_sem=send_sem.at[index],
            recv_sem=recv_sem.at[index], device_id=target, device_id_type=MESH,
        )
        copy.start()
        copies.append(copy)
    for copy in copies:
        copy.wait()


def widened(fields):
    both = jnp.stack(fields)
    top, bottom = both[:, :, 0], both[:, :, -1]
    pieces = (
        top, bottom, both[:, :, :, 0], both[:, :, :, -1],
        top[:, :, 0], top[:, :, -1], bottom[:, :, 0], bottom[:, :, -1],
    )
    landed = pl.pallas_call(
        functools.partial(halo_kernel, lax.axis_size("lat"), lax.axis_size("lon")),
        out_shape=tuple(jax.ShapeDtypeStruct(p.shape, p.dtype) for p in pieces),
        in_specs=[pl.BlockSpec(memory_space=pltpu.VMEM)] * 8,
        out_specs=(pl.BlockSpec(memory_space=pltpu.VMEM),) * 8,
        scratch_shapes=[pltpu.SemaphoreType.DMA((8,)), pltpu.SemaphoreType.DMA((8,))],
        compiler_params=pltpu.CompilerParams(
            collective_id=1, has_side_effects=True, vmem_limit_bytes=24 * 1024 * 1024
        ),
        name="halo",
    )(*pieces)
    below, above, east, west, below_east, below_west, above_east, above_west = landed

    def row(start, middle, end):
        return jnp.concatenate([start[:, None, None], middle[:, None], end[:, None, None]], axis=2)

    wide = []
    for index, field in enumerate(fields):
        middle = jnp.concatenate(
            [west[index][:, :, None], field, east[index][:, :, None]], axis=2
        )
        first = row(above_west[index], above[index], above_east[index])
        last = row(below_west[index], below[index], below_east[index])
        wide.append(mask_poles(jnp.concatenate([first, middle, last], axis=1)))
    return wide


def mask_poles(wide_field):
    lat_index = lax.axis_index("lat")
    lat_count = lax.axis_size("lat")
    total_rows = wide_field.shape[1]
    row_ids = lax.broadcasted_iota(jnp.int32, (1, total_rows, 1, 1), 1)
    upper = jnp.logical_and(row_ids == 0, lat_index == 0)
    lower = jnp.logical_and(row_ids == total_rows - 1, lat_index == lat_count - 1)
    return jnp.where(jnp.logical_or(upper, lower), jnp.zeros((), wide_field.dtype), wide_field)


def input_taps(act_wide, grad_flat, lat_rows, lon_cols):

    def input_compute(first_row, row_count):
        tap_parts = []
        for tap_index in range(9):
            row_off, col_off = divmod(tap_index, 3)
            tap_slab = act_wide[
                :, row_off : row_off + lat_rows, col_off : col_off + lon_cols, :
            ].reshape(-1, row_count)
            tap_parts.append(
                lax.dot_general(
                    tap_slab,
                    grad_flat,
                    (((0,), (0,)), ((), ())),
                    preferred_element_type=jnp.float32,
                )
            )
        return jnp.stack(tap_parts, axis=1)

    return input_compute


def reduce_update_gather(
    n_lat, n_q, max_norm, part, master, one, two,
    gathered, new_master, new_one, new_two, clipped,
    core_in, sums, right_in, left_in, lat_out, lat_in, norm_out, norm_in,
    send_sem, recv_sem,
):
    lat = lax.axis_index("lat")
    lon = lax.axis_index("lon")
    core = lax.rem(lon, 2)
    q = lon // 2
    hops = n_q // 2
    half = n_lat // 2
    counter = [0]
    pending = []

    def at(lat_id, q_id, core_id):
        return (lat_id, q_id * 2 + core_id)

    partner = at(lat, q, 1 - core)
    right_q = lax.rem(q + 1, n_q)
    left_q = lax.rem(q + n_q - 1, n_q)
    right, left = at(lat, right_q, core), at(lat, left_q, core)
    q_peers = [at(lat, lax.rem(q + d, n_q), core) for d in range(1, n_q)]
    lat_peers = [at(lax.rem(lat + d, n_lat), q, core) for d in range(1, n_lat)]

    def send(src, dst, target):
        index = counter[0]
        counter[0] += 1
        copy = pltpu.make_async_remote_copy(
            src_ref=src, dst_ref=dst, send_sem=send_sem.at[index],
            recv_sem=recv_sem.at[index], device_id=target, device_id_type=MESH,
        )
        copy.start()
        pending.append(copy)
        return copy

    def wrap(index, size):
        return lax.rem(index + size, size)

    barrier = pltpu.get_barrier_semaphore()
    greeted = [partner] + q_peers + lat_peers
    for device in greeted:
        pl.semaphore_signal(barrier, inc=1, device_id=device, device_id_type=MESH)
    pl.semaphore_wait(barrier, len(greeted))

    order = []
    for step in range(hops):
        for block in (hops - step, -hops + step):
            if block % n_q not in order:
                order.append(block % n_q)
    order.append(0)
    core_copies = []
    for offset in order:
        block = lax.rem(q + offset, n_q)
        core_copies.append(
            send(part.at[:, :, block, 1 - core], core_in.at[:, :, block], partner)
        )
    arrived = {}

    def core_sum(offset):
        if offset in arrived:
            return
        arrived[offset] = True
        core_copies[order.index(offset)].wait_recv()
        block = lax.rem(q + offset, n_q)

        @pl.loop(0, n_lat)
        def _(row):
            sums[block, row] = (
                part[:, row, block, core] + core_in[:, row, block]
            ).astype(jnp.bfloat16)

    def add_into(block, low, high, source):
        @pl.loop(low, high)
        def _(row):
            sums[block, row] = (
                sums[block, row].astype(jnp.float32) + source[row].astype(jnp.float32)
            ).astype(jnp.bfloat16)

    ring = []
    for step in range(hops):
        right_off = (hops - step) % n_q
        left_off = (step - hops) % n_q
        core_sum(right_off)
        core_sum(left_off)
        right_block = lax.rem(q + right_off, n_q)
        left_block = lax.rem(q + left_off, n_q)
        if step == 0:
            ring.append((
                send(sums.at[right_block, pl.ds(0, half)], right_in.at[0, pl.ds(0, half)], right),
                send(sums.at[left_block, pl.ds(half, n_lat - half)],
                     left_in.at[0, pl.ds(half, n_lat - half)], left),
            ))
        else:
            from_left, from_right = ring[-1]
            bounds = (0, half, half, n_lat) if step == 1 else (0, n_lat, 0, n_lat)
            from_left.wait_recv()
            add_into(right_block, bounds[0], bounds[1], right_in.at[step - 1])
            going_right = send(sums.at[right_block], right_in.at[step], right)
            from_right.wait_recv()
            add_into(left_block, bounds[2], bounds[3], left_in.at[step - 1])
            ring.append((going_right, send(sums.at[left_block], left_in.at[step], left)))
    core_sum(0)
    for copy in ring[-1]:
        copy.wait_recv()

    def q_total(row):
        total = part[:, row, q, core] + core_in[:, row, q]
        if hops > 1:
            return (
                total + right_in[hops - 1, row].astype(jnp.float32)
                + left_in[hops - 1, row].astype(jnp.float32)
            )
        return total + jnp.where(
            row < half, right_in[0, row].astype(jnp.float32), left_in[0, row].astype(jnp.float32)
        )

    lat_copies = []
    for step in range(1, n_lat):
        target = lax.rem(lat + step, n_lat)
        lat_out[step - 1] = q_total(target).astype(jnp.bfloat16)
        lat_copies.append(send(lat_out.at[step - 1], lat_in.at[step - 1], lat_peers[step - 1]))
    grad = q_total(lat)
    for step, copy in enumerate(lat_copies):
        copy.wait_recv()
        grad = grad + lat_in[step].astype(jnp.float32)
    clipped[...] = grad

    square = jnp.sum(grad * grad)
    slot = 0
    for stage, peers in enumerate(([partner], q_peers, lat_peers)):
        norm_out[stage] = jnp.full(norm_out.shape[1:], square, jnp.float32)
        copies = []
        for target in peers:
            copies.append(send(norm_out.at[stage], norm_in.at[slot], target))
            slot += 1
        tile = norm_out[stage]
        for index, copy in enumerate(copies):
            copy.wait_recv()
            tile = tile + norm_in[slot - len(peers) + index]
        square = jnp.max(tile)
    square = jnp.full((1, 1), square, jnp.float32)
    clip_factor = jnp.minimum(1.0, max_norm / (jnp.sqrt(square) + norm_eps))

    @pl.loop(0, clipped.shape[0])
    def _(tap):
        scaled = clip_factor * clipped[tap]
        clipped[tap] = scaled
        first = beta_one * one[tap] + (1.0 - beta_one) * scaled
        second = beta_two * two[tap] + (1.0 - beta_two) * scaled * scaled
        new_one[tap] = first
        new_two[tap] = second
        first_hat = first / (1.0 - beta_one**step_count)
        second_hat = second / (1.0 - beta_two**step_count)
        updated = master[tap] - learn_rate * (
            first_hat / (jnp.sqrt(second_hat) + adam_eps) + decay_rate * master[tap]
        )
        new_master[tap] = updated
        gathered[core, q, lat, tap] = updated.astype(jnp.bfloat16)

    copies = [
        send(gathered.at[core, q, lat], gathered.at[core, q, lat], peer) for peer in lat_peers
    ]
    for copy in copies:
        copy.wait_recv()
    core_in_copies = []

    def to_partner(block, low, count):
        piece = gathered.at[core, block, pl.ds(low, count)]
        core_in_copies.append(send(piece, piece, partner))

    from_left = from_right = None
    for step in range(hops):
        last = step == hops - 1
        right_block = wrap(q - step, n_q)
        left_block = lax.rem(q + step, n_q)
        if from_left is not None:
            from_left.wait_recv()
        piece = gathered.at[core, right_block, pl.ds(0, half if last else n_lat)]
        going_right = send(piece, piece, right)
        if from_right is not None:
            from_right.wait_recv()
        low = half if last else 0
        piece = gathered.at[core, left_block, pl.ds(low, n_lat - low)]
        going_left = send(piece, piece, left)
        to_partner(right_block, 0, n_lat)
        if step > 0:
            to_partner(left_block, 0, n_lat)
        from_left, from_right = going_right, going_left
    far = lax.rem(q + hops, n_q)
    from_left.wait_recv()
    to_partner(far, 0, half)
    from_right.wait_recv()
    to_partner(far, half, n_lat - half)
    for copy in core_in_copies:
        copy.wait_recv()
    for copy in pending:
        copy.wait_send()


def fused_update(partial, master, one, two):
    n_lat, n_q = lax.axis_size("lat"), lax.axis_size("lon") // 2
    taps, rows, width = master.shape
    part = partial.reshape(taps, n_lat, n_q, 2, rows, width)
    max_norm = math.sqrt(float(partial.size))
    shard = jax.ShapeDtypeStruct(master.shape, jnp.float32)
    hops = n_q // 2
    half_type = jnp.bfloat16
    block = (n_lat, taps, rows, width)
    peers = n_q + n_lat - 1
    vmem = pl.BlockSpec(memory_space=pltpu.VMEM)
    copies = 64 + 8 * (n_q + n_lat)
    return pl.pallas_call(
        functools.partial(reduce_update_gather, n_lat, n_q, max_norm),
        out_shape=(
            jax.ShapeDtypeStruct((2, n_q) + block, half_type), shard, shard, shard, shard,
        ),
        in_specs=[vmem] * 4,
        out_specs=(vmem,) * 5,
        scratch_shapes=[
            pltpu.VMEM((taps, n_lat, n_q, rows, width), jnp.float32),
            pltpu.VMEM((n_q,) + block, half_type),
            pltpu.VMEM((hops,) + block, half_type),
            pltpu.VMEM((hops,) + block, half_type),
            pltpu.VMEM((n_lat - 1, taps, rows, width), half_type),
            pltpu.VMEM((n_lat - 1, taps, rows, width), half_type),
            pltpu.VMEM((3, 8, 128), jnp.float32),
            pltpu.VMEM((peers, 8, 128), jnp.float32),
            pltpu.SemaphoreType.DMA((copies,)),
            pltpu.SemaphoreType.DMA((copies,)),
        ],
        compiler_params=pltpu.CompilerParams(
            collective_id=0, has_side_effects=True, vmem_limit_bytes=60 * 1024 * 1024
        ),
        name="reduce_update_gather",
    )(part, master, one, two)


def per_device(activations, upstream, master, moment_one, moment_two):
    lat_rows = activations.shape[1]
    lon_cols = activations.shape[2]
    grad_flat = upstream.reshape(-1, upstream.shape[3])
    old_weights = master[:, ::-1].astype(jnp.bfloat16)
    old_full = lax.all_gather(old_weights, ("lat", "lon"), axis=0, tiled=True)
    act_wide, grad_wide = widened((activations, upstream))
    term_maker = input_taps(act_wide, grad_flat, lat_rows, lon_cols)
    partial = term_maker(jnp.int32(0), activations.shape[3])

    def by_tap(array):
        return jnp.transpose(array, (1, 0, 2))

    gathered, new_master, new_one, new_two, clipped = fused_update(
        by_tap(partial), by_tap(master), by_tap(moment_one), by_tap(moment_two)
    )
    new_weights = jnp.transpose(gathered, (2, 1, 0, 4, 3, 5)).reshape(
        activations.shape[3], gathered.shape[3], gathered.shape[5]
    )
    old_full, new_one = lax.optimization_barrier((old_full, new_one))
    input_grad = lax.conv_general_dilated(
        grad_wide,
        old_full.reshape(old_full.shape[0], 3, 3, old_full.shape[2]),
        (1, 1),
        "VALID",
        dimension_numbers=("NHWC", "OHWI", "NHWC"),
        preferred_element_type=jnp.float32,
    ).astype(jnp.bfloat16)
    return (
        input_grad, new_weights, by_tap(new_master), by_tap(new_one), by_tap(new_two),
        by_tap(clipped),
    )


def solution(mesh):
    in_specs = (
        P(None, "lat", "lon", None),
        P(None, "lat", "lon", None),
        P(("lat", "lon"), None, None),
        P(("lat", "lon"), None, None),
        P(("lat", "lon"), None, None),
    )
    out_specs = (
        P(None, "lat", "lon", None),
        P(),
        P(("lat", "lon"), None, None),
        P(("lat", "lon"), None, None),
        P(("lat", "lon"), None, None),
        P(("lat", "lon"), None, None),
    )
    return jax.shard_map(
        per_device, mesh=mesh, in_specs=in_specs, out_specs=out_specs, check_vma=False
    )
```
